16 devices in a mesh: col: 2 (over z), row: 8 (over y, x, core).
Axes of the slice: x: 2, y: 2, z: 2, core: 2. Of those that a mesh axis runs over, the one named last changes fastest.
Arguments:
- adjacency: bfloat16 [24576, 24576], P('row', 'col')
- pers_vec: float32 [24576, 64], P(('row', 'col'))
- restart_wt: float32 [16, 64], replicated
Outputs:
- output 1: float32 [24576, 64], P(('col', 'row'))
- output 2: float32 [24576, 64], P(('row', 'col'))
All inputs are finite; a program needn't handle non-finite values.
Results may differ from the reference program's by a relative error of at most 0.001.
Values are sent between devices in bfloat16 or wider.
A program may use at most 1 GiB of HBM per device.

```python
import jax
import jax.numpy as jnp
from jax import lax

N = 24576
DEG = 8
M = 64
SWEEPS = 16


def setup_inputs(seed: int = 0) -> dict:
    base_key = jax.random.key(seed)
    k_out, k_pop, k_adj, k_start, k_val, k_rest = jax.random.split(base_key, 6)
    out_budget = jax.random.randint(k_out, (N,), 1, 2 * DEG + 1)
    popularity = jax.random.randint(k_pop, (N,), 1, 16)
    row_count = N // 16

    def draw_rows(block_idx):
        draw_bits = jax.random.randint(jax.random.fold_in(k_adj, block_idx), (row_count, N), 0, 8 * N)
        pop_rows = lax.dynamic_slice(popularity, (block_idx * row_count,), (row_count,))
        return (draw_bits < pop_rows[:, None] * out_budget[None, :]).astype(jnp.bfloat16)

    adjacency = lax.map(draw_rows, jnp.arange(16)).reshape(N, N)
    win_start = jax.random.randint(k_start, (M,), 0, N)
    inside = ((jnp.arange(N)[:, None] - win_start[None, :]) % N) < (N // 8)
    raw_vals = jnp.abs(jax.random.normal(k_val, (N, M), jnp.float32)) * jnp.where(inside, 1.0, 0.05)
    pers_vec = raw_vals * lax.rsqrt(jnp.mean(raw_vals * raw_vals, axis=0, keepdims=True))
    restart_wt = jax.random.uniform(k_rest, (SWEEPS, M), jnp.float32, 0.15, 0.45)
    return {"adjacency": adjacency, "pers_vec": pers_vec, "restart_wt": restart_wt}


def col_normalise(vals):
    return vals * lax.rsqrt(jnp.mean(vals * vals, axis=0, keepdims=True))


def reference(adjacency, pers_vec, restart_wt):
    def sweep(carry, weight):
        hub_vec = carry[0]
        auth_prod = lax.dot_general(adjacency, hub_vec.astype(jnp.bfloat16), (((0,), (0,)), ((), ())), preferred_element_type=jnp.float32)
        auth_vec = col_normalise(auth_prod)
        hub_prod = jnp.dot(adjacency, auth_vec.astype(jnp.bfloat16), preferred_element_type=jnp.float32)
        hub_new = (1.0 - weight) * col_normalise(hub_prod) + weight * pers_vec
        return (hub_new, auth_vec), None

    final_state, unused_out = lax.scan(sweep, (pers_vec, jnp.zeros_like(pers_vec)), restart_wt)
    return final_state[1], final_state[0]
```

```python
import functools

import jax
import jax.numpy as jnp
from jax import lax
from jax.experimental import pallas as pl
from jax.experimental.pallas import tpu as pltpu
from jax.sharding import PartitionSpec as P

F32, BF16 = jnp.float32, jnp.bfloat16
MESH = pl.DeviceIdType.MESH
SLOTS = 6


def prod_cols(lhs, rhs):
    return lax.dot_general(lhs, rhs, (((1,), (0,)), ((), ())), preferred_element_type=F32)


def prod_rows(lhs, rhs):
    return lax.dot_general(lhs, rhs, (((1,), (1,)), ((), ())), preferred_element_type=F32)


def lane_tile(v, width):
    return jnp.concatenate([v] * (width // 128), axis=1)


def square_sums(parts):
    total = None
    for part in parts:
        for t in range(part.shape[1] // 128):
            v = part[:, t * 128:(t + 1) * 128]
            total = v * v if total is None else total + v * v
    full = jnp.concatenate([total, jnp.zeros((128 - total.shape[0], 128), F32)], axis=0)
    row = jnp.sum(full.T, axis=0, keepdims=True)
    return jnp.broadcast_to(row, (8, 128))


def kernel(n_total, v_ref, b_ref, a_hbm, auth_out, hub_out,
           res, stm, hb, ab, acc, hub, rd, s1x, s1y, s2x, s2y, zr, sq_send, sq1, sq2,
           res_sem, stm_sem, dd_s, dd_r, x1_s, x1_r, y1_s, y1_r, x2_s, x2_r, y2_s, y2_r,
           ag_s, ag_r, z_s, z_r, h_s, h_r, q1_s, q1_r, q2_s, q2_r):
    sweeps, dim = b_ref.shape[0], v_ref.shape[0]
    rows, width = stm.shape[1], stm.shape[2]
    j, i = lax.axis_index("col"), lax.axis_index("row")
    core, x, y = i % 2, (i // 2) % 2, i // 4
    partner = {"row": i + 1 - 2 * core, "col": j}
    xnb = {"row": i + 2 - 4 * x, "col": j}
    ynb = {"row": i + 4 - 8 * y, "col": j}
    znb = {"row": i, "col": 1 - j}
    base_o, base_x = 4 * y + 2 * x, 4 * y + 2 * (1 - x)
    base_y, base_d = 4 * (1 - y) + 2 * x, 4 * (1 - y) + 2 * (1 - x)
    mine, other = core, 1 - core
    ord1 = [base_d + other, base_d + mine, base_x + other, base_x + mine,
            base_y + other, base_y + mine, base_o + other, base_o + mine]
    ord2 = [base_o + other, base_o + mine, base_x + mine, base_y + mine,
            base_x + other, base_y + other, base_d + other, base_d + mine]

    def rcopy(src, dst, s, r, dev):
        return pltpu.make_async_remote_copy(src, dst, s, r, device_id=dev, device_id_type=MESH)

    def a_block(which, chunk, half):
        return a_hbm.at[pl.ds(pl.multiple_of(which * rows, rows), rows),
                        pl.ds(pl.multiple_of((chunk * 2 + half) * width, width), width)]

    def load(chunk, half, slot):
        return pltpu.make_async_copy(a_block(1 - j, chunk, half), stm.at[slot], stm_sem.at[slot])

    def load_res(u):
        return pltpu.make_async_copy(a_block(j, u // 2, u % 2), res.at[u // 2, u % 2], res_sem.at[u])

    def stream_unit(ci, half, order, after):
        slot = (2 * ci + half) % SLOTS
        if ci >= 2:
            load(order[ci], half, slot).wait()

        def done():
            if ci <= 4:
                load(order[ci + 3], half, slot).start()
            elif ci == 5:
                load(after[2], half, slot).start()
        return slot, done

    def copies_h():
        return rcopy(hb.at[0], hb.at[1], h_s, h_r, znb)

    def all_sum(row8, buf, send, recv):
        sq_send[...] = row8
        buf[0] = row8
        copies = []
        for d in range(15, 0, -1):
            dz, dy, dx, dc = d // 8, (d // 4) % 2, (d // 2) % 2, d % 2
            dev = {"row": 4 * ((y + dy) % 2) + 2 * ((x + dx) % 2) + (core + dc) % 2, "col": (j + dz) % 2}
            copies.append(rcopy(sq_send, buf.at[d], send.at[d], recv.at[d], dev))
            copies[-1].start()
        for c in copies:
            c.wait_recv()
        vals = [buf[d] for d in range(16)]
        while len(vals) > 1:
            vals = [vals[q] + vals[q + 1] for q in range(0, len(vals), 2)]
        scale = lax.rsqrt(vals[0] / n_total)
        cols = jnp.concatenate([scale] * 16, axis=0).T[:dim]
        for c in copies:
            c.wait_send()
        return cols

    for u in range(16):
        load_res(u).start()
    for u in range(SLOTS):
        load(ord1[u // 2], u % 2, u).start()
    hb[0] = v_ref[...].astype(BF16)
    copies_h().start()
    for u in range(16):
        load_res(u).wait()
    for u in range(4):
        load(ord1[u // 2], u % 2, u).wait()

    def sweep(k, carry):
        def own(u, c):
            acc[u // 2, u % 2] = prod_cols(hb[0], res[u // 2, u % 2])
            return c
        lax.fori_loop(0, 16, own, 0)
        h_cp = copies_h()
        h_cp.wait_recv()

        dd = [rcopy(acc.at[ord1[2 * t]], rd.at[t], dd_s.at[t], dd_r.at[t], partner) for t in range(4)]
        d_mine, x_mine, y_mine, o_mine = ord1[1], ord1[3], ord1[5], ord1[7]
        x1 = [rcopy(acc.at[d_mine, 0], s1x.at[0], x1_s.at[0], x1_r.at[0], xnb),
              rcopy(acc.at[x_mine, 0], s1x.at[1], x1_s.at[1], x1_r.at[1], xnb)]
        y1 = [rcopy(acc.at[d_mine, 1], s1y.at[0], y1_s.at[0], y1_r.at[0], ynb),
              rcopy(acc.at[y_mine, 1], s1y.at[1], y1_s.at[1], y1_r.at[1], ynb)]
        x2 = rcopy(acc.at[x_mine, 1], s2x, x2_s, x2_r, xnb)
        y2 = rcopy(acc.at[y_mine, 0], s2y, y2_s, y2_r, ynb)

        def other_rows(ci):
            chunk = ord1[ci]

            def unit(half, c):
                slot, done = stream_unit(ci, half, ord1, ord2)
                acc[chunk, half] += prod_cols(hb[1], stm[slot])
                done()
                return c
            lax.fori_loop(0, 2, unit, 0)

        def combine(t):
            dd[t].wait_recv()
            m = ord1[2 * t + 1]
            acc[m] += rd[t]

        other_rows(0)
        dd[0].start()
        other_rows(1)
        other_rows(2)
        dd[1].start()
        combine(0)
        x1[0].start()
        y1[0].start()
        other_rows(3)
        other_rows(4)
        dd[2].start()
        combine(1)
        x1[1].start()
        other_rows(5)
        other_rows(6)
        dd[3].start()
        combine(2)
        y1[1].start()
        other_rows(7)
        x1[0].wait_recv()
        acc[y_mine, 0] += s1x[0]
        y2.start()
        y1[0].wait_recv()
        acc[x_mine, 1] += s1y[0]
        x2.start()
        combine(3)
        x1[1].wait_recv()
        y1[1].wait_recv()
        p0 = acc[o_mine, 0] + s1x[1]
        p1 = acc[o_mine, 1] + s1y[1]
        acc[o_mine, 0] = p0
        acc[o_mine, 1] = p1
        y2.wait_recv()
        x2.wait_recv()
        p0 = acc[o_mine, 0] + s2y[...]
        p1 = acc[o_mine, 1] + s2x[...]
        auth_out[0] = p0
        auth_out[1] = p1
        scale = all_sum(square_sums([p0, p1]), sq1, q1_s, q1_r)
        wide = lane_tile(scale, width)
        for half in range(2):
            val = auth_out[half] * wide
            auth_out[half] = val
            ab[i, half] = val.astype(BF16)
        for c in dd + x1 + y1 + [x2, y2, h_cp]:
            c.wait_send()

        px, py, pd = ord1[3], ord1[5], ord1[1]
        to_p = rcopy(ab.at[i], ab.at[i], ag_s.at[0], ag_r.at[0], partner)
        to_x = [rcopy(ab.at[i, h], ab.at[i, h], ag_s.at[1 + h], ag_r.at[1 + h], xnb) for h in range(2)]
        to_y = [rcopy(ab.at[i, h], ab.at[i, h], ag_s.at[3 + h], ag_r.at[3 + h], ynb) for h in range(2)]
        rel_y = rcopy(ab.at[px, 0], ab.at[px, 0], ag_s.at[5], ag_r.at[5], ynb)
        rel_x = rcopy(ab.at[py, 1], ab.at[py, 1], ag_s.at[6], ag_r.at[6], xnb)
        fw_x = rcopy(ab.at[px], ab.at[px], ag_s.at[7], ag_r.at[7], partner)
        fw_y = rcopy(ab.at[py], ab.at[py], ag_s.at[8], ag_r.at[8], partner)
        fw_d = rcopy(ab.at[pd], ab.at[pd], ag_s.at[9], ag_r.at[9], partner)
        to_p.start()
        to_x[0].start()
        to_y[1].start()
        to_x[1].start()
        to_y[0].start()

        def resident(chunk, first):
            def unit(half, c):
                val = prod_rows(ab[chunk, half], res[chunk, half])
                if first:
                    @pl.when(half == 0)
                    def _():
                        hub[0] = val

                    @pl.when(half != 0)
                    def _():
                        hub[0] += val
                else:
                    hub[0] += val
                return c
            lax.fori_loop(0, 2, unit, 0)

        def streamed(ci):
            chunk = ord2[ci]

            def unit(half, c):
                slot, done = stream_unit(ci, half, ord2, ord1)
                hub[1] += prod_rows(ab[chunk, half], stm[slot])
                done()
                return c
            lax.fori_loop(0, 2, unit, 0)

        hub[0] = jnp.zeros(hub.shape[1:], F32)
        hub[1] = jnp.zeros(hub.shape[1:], F32)
        resident(ord2[1], False)
        streamed(1)
        to_p.wait_recv()
        resident(ord2[0], False)
        streamed(0)
        to_x[0].wait_recv()
        rel_y.start()
        to_y[1].wait_recv()
        rel_x.start()
        to_x[1].wait_recv()
        fw_x.start()
        to_y[0].wait_recv()
        fw_y.start()
        streamed(2)
        streamed(3)
        fw_x.wait_recv()
        streamed(4)
        rel_y.wait_recv()
        rel_x.wait_recv()
        fw_d.start()
        fw_y.wait_recv()
        streamed(5)
        fw_d.wait_recv()
        streamed(6)
        streamed(7)
        z_cp = rcopy(hub.at[1], zr, z_s, z_r, znb)
        z_cp.start()

        def rest(u, c):
            chunk = (base_o + 2 + u // 2) % 8
            half = u % 2
            hub[0] += prod_rows(ab[chunk, half], res[chunk, half])
            return c
        lax.fori_loop(0, 12, rest, 0)
        z_cp.wait_recv()
        val = hub[0] + zr[...]
        hub[0] = val
        scale = all_sum(square_sums([val]), sq2, q2_s, q2_r)
        wt = b_ref[k]
        keep = lane_tile((1.0 - wt) * 1.0, 2 * width)
        hv = keep * (hub[0] * lane_tile(scale, 2 * width)) + lane_tile(wt, 2 * width) * v_ref[...]
        hub_out[...] = hv
        hb[0] = hv.astype(BF16)
        for c in [to_p, *to_x, *to_y, rel_y, rel_x, fw_x, fw_y, fw_d, z_cp]:
            c.wait_send()

        @pl.when(k < sweeps - 1)
        def _():
            copies_h().start()
        return carry

    lax.fori_loop(0, sweeps, sweep, 0)
    for half in range(2):
        load(ord1[2], half, 4 + half).wait()


def solution(mesh):
    def device_fn(adj_tile, pers_piece, restart_wt):
        sweeps, dim = restart_wt.shape
        chunk = pers_piece.shape[0]
        width = chunk // 2
        n_total = float(chunk * mesh.size)
        wt = jnp.broadcast_to(restart_wt[:, :, None], (sweeps, dim, 128))
        vmem = pl.BlockSpec(memory_space=pltpu.VMEM)
        dma = pltpu.SemaphoreType.DMA
        auth, hub = pl.pallas_call(
            functools.partial(kernel, n_total),
            out_shape=(jax.ShapeDtypeStruct((2, dim, width), F32), jax.ShapeDtypeStruct((dim, chunk), F32)),
            in_specs=[vmem, vmem, pl.BlockSpec(memory_space=pl.ANY)],
            out_specs=(vmem, vmem),
            scratch_shapes=[
                pltpu.VMEM((8, 2, chunk, width), BF16),
                pltpu.VMEM((SLOTS, chunk, width), BF16),
                pltpu.VMEM((2, dim, chunk), BF16),
                pltpu.VMEM((8, 2, dim, width), BF16),
                pltpu.VMEM((8, 2, dim, width), F32),
                pltpu.VMEM((2, dim, chunk), F32),
                pltpu.VMEM((4, 2, dim, width), F32),
                pltpu.VMEM((2, dim, width), F32),
                pltpu.VMEM((2, dim, width), F32),
                pltpu.VMEM((dim, width), F32),
                pltpu.VMEM((dim, width), F32),
                pltpu.VMEM((dim, chunk), F32),
                pltpu.VMEM((8, 128), F32),
                pltpu.VMEM((16, 8, 128), F32),
                pltpu.VMEM((16, 8, 128), F32),
                dma((16,)), dma((SLOTS,)), dma((4,)), dma((4,)), dma((2,)), dma((2,)), dma((2,)), dma((2,)),
                dma, dma, dma, dma, dma((10,)), dma((10,)), dma, dma, dma, dma,
                dma((16,)), dma((16,)), dma((16,)), dma((16,)),
            ],
            compiler_params=pltpu.CompilerParams(vmem_limit_bytes=67043328, has_side_effects=True),
        )(pers_piece.T, wt, adj_tile)
        return auth.transpose(0, 2, 1).reshape(chunk, dim), hub.T

    return jax.shard_map(
        device_fn, mesh=mesh,
        in_specs=(P("row", "col"), P(("row", "col"), None), P(None, None)),
        out_specs=(P(("col", "row"), None), P(("row", "col"), None)), check_vma=False)
```

```python
import functools

import jax
import jax.numpy as jnp
from jax import lax
from jax.experimental import pallas as pl
from jax.experimental.pallas import tpu as pltpu
from jax.sharding import PartitionSpec as P

F32, BF16 = jnp.float32, jnp.bfloat16
MESH = pl.DeviceIdType.MESH
SLOTS = 6


def prod_cols(lhs, rhs):
    return lax.dot_general(lhs, rhs, (((1,), (0,)), ((), ())), preferred_element_type=F32)


def prod_rows(lhs, rhs):
    return lax.dot_general(lhs, rhs, (((1,), (1,)), ((), ())), preferred_element_type=F32)


def lane_tile(v, width):
    return jnp.concatenate([v] * (width // 128), axis=1)


def row_to_lanes(row, dim):
    return jnp.broadcast_to(row, (128, 128)).T[:dim]


def square_sums(parts):
    total = None
    for part in parts:
        for t in range(part.shape[1] // 128):
            v = part[:, t * 128:(t + 1) * 128]
            total = v * v if total is None else total + v * v
    full = jnp.concatenate([total, jnp.zeros((128 - total.shape[0], 128), F32)], axis=0)
    row = jnp.sum(full.T, axis=0, keepdims=True)
    return jnp.broadcast_to(row, (8, 128))


def kernel(n_total, v_ref, b_ref, a_hbm, auth_out, hub_out,
           res, stm, vt, bt, hb, ab, acc, own_sum, oth_sum, rd, s1x, s1y, s2x, s2y, zr, sq_send, sq1, sq2,
           res_sem, stm_sem, dd_s, dd_r, x1_s, x1_r, y1_s, y1_r, x2_s, x2_r, y2_s, y2_r,
           ag_s, ag_r, z_s, z_r, h_s, h_r, q1_s, q1_r, q2_s, q2_r):
    sweeps, dim = b_ref.shape
    rows, width = stm.shape[1], stm.shape[2]
    groups, span = oth_sum.shape[0], oth_sum.shape[2]
    j, i = lax.axis_index("col"), lax.axis_index("row")
    core, x, y = i % 2, (i // 2) % 2, i // 4
    partner = {"row": i + 1 - 2 * core, "col": j}
    xnb = {"row": i + 2 - 4 * x, "col": j}
    ynb = {"row": i + 4 - 8 * y, "col": j}
    znb = {"row": i, "col": 1 - j}
    base_o, base_x = 4 * y + 2 * x, 4 * y + 2 * (1 - x)
    base_y, base_d = 4 * (1 - y) + 2 * x, 4 * (1 - y) + 2 * (1 - x)
    mine, other = core, 1 - core
    ord1 = [base_d + other, base_d + mine, base_x + other, base_x + mine,
            base_y + other, base_y + mine, base_o + other, base_o + mine]
    ord2 = [base_o + other, base_o + mine, base_x + mine, base_y + mine,
            base_x + other, base_y + other, base_d + other, base_d + mine]

    def rcopy(src, dst, s, r, dev):
        return pltpu.make_async_remote_copy(src, dst, s, r, device_id=dev, device_id_type=MESH)

    def a_block(which, chunk, half):
        return a_hbm.at[pl.ds(pl.multiple_of(which * rows, rows), rows),
                        pl.ds(pl.multiple_of((chunk * 2 + half) * width, width), width)]

    def load(chunk, half, slot):
        return pltpu.make_async_copy(a_block(1 - j, chunk, half), stm.at[slot], stm_sem.at[slot])

    def load_res(u):
        return pltpu.make_async_copy(a_block(j, u // 2, u % 2), res.at[u // 2, u % 2], res_sem.at[u])

    def block_wait(ci, order):
        slots = [(2 * ci + half) % SLOTS for half in range(2)]
        if ci >= 2:
            for half in range(2):
                load(order[ci], half, slots[half]).wait()
        return slots

    def block_next(ci, order, after):
        for half in range(2):
            slot = (2 * ci + half) % SLOTS
            if ci <= 4:
                load(order[ci + 3], half, slot).start()
            elif ci == 5:
                load(after[2], half, slot).start()

    def copies_h():
        return rcopy(hb.at[0], hb.at[1], h_s, h_r, znb)

    def all_sum(row8, buf, send, recv):
        sq_send[...] = row8
        buf[0] = row8
        copies = []
        for d in range(15, 0, -1):
            dz, dy, dx, dc = d // 8, (d // 4) % 2, (d // 2) % 2, d % 2
            dev = {"row": 4 * ((y + dy) % 2) + 2 * ((x + dx) % 2) + (core + dc) % 2, "col": (j + dz) % 2}
            copies.append(rcopy(sq_send, buf.at[d], send.at[d], recv.at[d], dev))
            copies[-1].start()
        for c in copies:
            c.wait_recv()
        vals = [buf[d] for d in range(16)]
        while len(vals) > 1:
            vals = [vals[q] + vals[q + 1] for q in range(0, len(vals), 2)]
        scale = lax.rsqrt(vals[0] / n_total)
        cols = row_to_lanes(scale[:1], dim)
        for c in copies:
            c.wait_send()
        return cols

    for u in range(16):
        load_res(u).start()
    for u in range(SLOTS):
        load(ord1[u // 2], u % 2, u).start()
    barrier = pltpu.get_barrier_semaphore()
    for d in range(1, 16):
        dz, dy, dx, dc = d // 8, (d // 4) % 2, (d // 2) % 2, d % 2
        dev = {"row": 4 * ((y + dy) % 2) + 2 * ((x + dx) % 2) + (core + dc) % 2, "col": (j + dz) % 2}
        pl.semaphore_signal(barrier, inc=1, device_id=dev, device_id_type=MESH)
    pad = jnp.zeros((128, 128 - dim), F32)
    for t in range(rows // 128):
        tile = jnp.concatenate([v_ref[t * 128:(t + 1) * 128, :], pad], axis=1)
        vt[:, t * 128:(t + 1) * 128] = tile.T[:dim]
    hb[0] = vt[...].astype(BF16)
    pl.semaphore_wait(barrier, 15)
    copies_h().start()
    for k in range(sweeps):
        bt[k] = row_to_lanes(jnp.concatenate([b_ref[k:k + 1, :], pad[:1]], axis=1), dim)

    def first(c, carry):
        for half in range(2):
            load_res(2 * c + half).wait()
        for half in range(2):
            acc[c, half] = prod_cols(hb[0], res[c, half])
        return carry
    lax.fori_loop(0, 8, first, 0)
    for u in range(4):
        load(ord1[u // 2], u % 2, u).wait()

    def sweep(k, carry):
        with jax.named_scope("hwait"):
            h_cp = copies_h()
            h_cp.wait_recv()

        dd = [rcopy(acc.at[ord1[2 * t]], rd.at[t], dd_s.at[t], dd_r.at[t], partner) for t in range(4)]
        d_mine, x_mine, y_mine, o_mine = ord1[1], ord1[3], ord1[5], ord1[7]
        x1 = [rcopy(acc.at[d_mine, 0], s1x.at[0], x1_s.at[0], x1_r.at[0], xnb),
              rcopy(acc.at[x_mine, 0], s1x.at[1], x1_s.at[1], x1_r.at[1], xnb)]
        y1 = [rcopy(acc.at[d_mine, 1], s1y.at[0], y1_s.at[0], y1_r.at[0], ynb),
              rcopy(acc.at[y_mine, 1], s1y.at[1], y1_s.at[1], y1_r.at[1], ynb)]
        x2 = rcopy(acc.at[x_mine, 1], s2x, x2_s, x2_r, xnb)
        y2 = rcopy(acc.at[y_mine, 0], s2y, y2_s, y2_r, ynb)

        def other_rows(ci):
            chunk = ord1[ci]
            slots = block_wait(ci, ord1)
            for half in range(2):
                acc[chunk, half] += prod_cols(hb[1], stm[slots[half]])
            block_next(ci, ord1, ord2)

        def combine(t):
            dd[t].wait_recv()
            m = ord1[2 * t + 1]
            acc[m] += rd[t]

        with jax.named_scope("p1a"):
            other_rows(0)
            dd[0].start()
            other_rows(1)
            other_rows(2)
            dd[1].start()
        with jax.named_scope("comb0"):
            combine(0)
            x1[0].start()
            y1[0].start()
        with jax.named_scope("p1b"):
            other_rows(3)
            other_rows(4)
            dd[2].start()
        with jax.named_scope("comb1"):
            combine(1)
            x1[1].start()
        with jax.named_scope("p1c"):
            other_rows(5)
            other_rows(6)
            dd[3].start()
        with jax.named_scope("comb2"):
            combine(2)
            y1[1].start()
        with jax.named_scope("p1d"):
            other_rows(7)
        with jax.named_scope("rs2"):
            x1[0].wait_recv()
            acc[y_mine, 0] += s1x[0]
            y2.start()
            y1[0].wait_recv()
            acc[x_mine, 1] += s1y[0]
            x2.start()
        with jax.named_scope("rs3"):
            combine(3)
            x1[1].wait_recv()
            y1[1].wait_recv()
            p0 = acc[o_mine, 0] + s1x[1]
            p1 = acc[o_mine, 1] + s1y[1]
            acc[o_mine, 0] = p0
            acc[o_mine, 1] = p1
        with jax.named_scope("rs4"):
            y2.wait_recv()
            x2.wait_recv()
            p0 = acc[o_mine, 0] + s2y[...]
            p1 = acc[o_mine, 1] + s2x[...]
            auth_out[0] = p0
            auth_out[1] = p1
        with jax.named_scope("ar1"):
            scale = all_sum(square_sums([p0, p1]), sq1, q1_s, q1_r)
        with jax.named_scope("norm1"):
            wide = lane_tile(scale, width)
            for half in range(2):
                val = auth_out[half] * wide
                auth_out[half] = val
                ab[i, half] = val.astype(BF16)
            for c in dd + x1 + y1 + [x2, y2, h_cp]:
                c.wait_send()

        px, py, pd = ord1[3], ord1[5], ord1[1]
        to_p = rcopy(ab.at[i], ab.at[i], ag_s.at[0], ag_r.at[0], partner)
        to_x = [rcopy(ab.at[i, h], ab.at[i, h], ag_s.at[1 + h], ag_r.at[1 + h], xnb) for h in range(2)]
        to_y = [rcopy(ab.at[i, h], ab.at[i, h], ag_s.at[3 + h], ag_r.at[3 + h], ynb) for h in range(2)]
        rel_y = rcopy(ab.at[px, 0], ab.at[px, 0], ag_s.at[5], ag_r.at[5], ynb)
        rel_x = rcopy(ab.at[py, 1], ab.at[py, 1], ag_s.at[6], ag_r.at[6], xnb)
        fw_x = rcopy(ab.at[px], ab.at[px], ag_s.at[7], ag_r.at[7], partner)
        fw_y = rcopy(ab.at[py], ab.at[py], ag_s.at[8], ag_r.at[8], partner)
        fw_d = rcopy(ab.at[pd], ab.at[pd], ag_s.at[9], ag_r.at[9], partner)
        to_p.start()
        to_x[0].start()
        to_y[1].start()
        to_x[1].start()
        to_y[0].start()

        def resident(chunk):
            return prod_rows(ab[chunk, 0], res[chunk, 0]) + prod_rows(ab[chunk, 1], res[chunk, 1])

        def streamed(ci, first=False):
            chunk = ord2[ci]
            slots = block_wait(ci, ord2)
            val = prod_rows(ab[chunk, 0], stm[slots[0]]) + prod_rows(ab[chunk, 1], stm[slots[1]])
            for g in range(groups):
                part = val[:, g * span:(g + 1) * span]
                if first:
                    oth_sum[g] = part
                else:
                    oth_sum[g] += part
            block_next(ci, ord2, ord1)

        with jax.named_scope("p2a"):
            own_sum[...] = resident(ord2[1])
            streamed(1, first=True)
        with jax.named_scope("p2b"):
            to_p.wait_recv()
            own_sum[...] += resident(ord2[0])
            streamed(0)
        with jax.named_scope("xwait"):
            to_x[0].wait_recv()
            rel_y.start()
            to_y[1].wait_recv()
            rel_x.start()
            to_x[1].wait_recv()
            fw_x.start()
            to_y[0].wait_recv()
            fw_y.start()
        with jax.named_scope("p2c"):
            streamed(2)
            streamed(3)
        with jax.named_scope("fxwait"):
            fw_x.wait_recv()
        with jax.named_scope("p2d"):
            streamed(4)
        with jax.named_scope("dwait"):
            rel_y.wait_recv()
            rel_x.wait_recv()
            fw_d.start()
            fw_y.wait_recv()
        with jax.named_scope("p2e"):
            streamed(5)
        with jax.named_scope("fdwait"):
            fw_d.wait_recv()
        with jax.named_scope("p2f"):
            slots = block_wait(6, ord2) + block_wait(7, ord2)
            z_cps = [rcopy(oth_sum.at[g], zr.at[g], z_s.at[g], z_r.at[g], znb) for g in range(groups)]
            for g in range(groups):
                val = oth_sum[g]
                for q in range(4):
                    val += prod_rows(ab[ord2[6 + q // 2], q % 2], stm[slots[q], g * span:(g + 1) * span, :])
                oth_sum[g] = val
                z_cps[g].start()

        with jax.named_scope("p2rest"):
            for q in range(6):
                own_sum[...] += resident((base_o + 2 + q) % 8)
        with jax.named_scope("zwait"):
            for g in range(groups):
                z_cps[g].wait_recv()
        with jax.named_scope("ar2"):
            val = own_sum[...] + jnp.concatenate([zr[g] for g in range(groups)], axis=1)
            own_sum[...] = val
            scale = all_sum(square_sums([val]), sq2, q2_s, q2_r)
        with jax.named_scope("upd"):
            wt = bt[k]
            hv = lane_tile(1.0 - wt, rows) * (own_sum[...] * lane_tile(scale, rows)) + lane_tile(wt, rows) * vt[...]
            hub_out[...] = hv
            hb[0] = hv.astype(BF16)
            for c in [to_p, *to_x, *to_y, rel_y, rel_x, fw_x, fw_y, fw_d, *z_cps]:
                c.wait_send()

        with jax.named_scope("own"):
            @pl.when(k < sweeps - 1)
            def _():
                copies_h().start()
                for u in range(16):
                    acc[u // 2, u % 2] = prod_cols(hb[0], res[u // 2, u % 2])
        return carry

    lax.fori_loop(0, sweeps, sweep, 0)
    for half in range(2):
        load(ord1[2], half, 4 + half).wait()


def solution(mesh):
    def device_fn(adj_tile, pers_piece, restart_wt):
        sweeps, dim = restart_wt.shape
        chunk = pers_piece.shape[0]
        width = chunk // 2
        n_total = float(chunk * mesh.size)
        groups = 3 if chunk % 384 == 0 else 2
        vmem = pl.BlockSpec(memory_space=pltpu.VMEM)
        dma = pltpu.SemaphoreType.DMA
        auth, hub = pl.pallas_call(
            functools.partial(kernel, n_total),
            out_shape=(jax.ShapeDtypeStruct((2, dim, width), F32), jax.ShapeDtypeStruct((dim, chunk), F32)),
            in_specs=[vmem, vmem, pl.BlockSpec(memory_space=pl.ANY)],
            out_specs=(vmem, vmem),
            scratch_shapes=[
                pltpu.VMEM((8, 2, chunk, width), BF16),
                pltpu.VMEM((SLOTS, chunk, width), BF16),
                pltpu.VMEM((dim, chunk), F32),
                pltpu.VMEM((sweeps, dim, 128), F32),
                pltpu.VMEM((2, dim, chunk), BF16),
                pltpu.VMEM((8, 2, dim, width), BF16),
                pltpu.VMEM((8, 2, dim, width), F32),
                pltpu.VMEM((dim, chunk), F32),
                pltpu.VMEM((groups, dim, chunk // groups), F32),
                pltpu.VMEM((4, 2, dim, width), F32),
                pltpu.VMEM((2, dim, width), F32),
                pltpu.VMEM((2, dim, width), F32),
                pltpu.VMEM((dim, width), F32),
                pltpu.VMEM((dim, width), F32),
                pltpu.VMEM((groups, dim, chunk // groups), F32),
                pltpu.VMEM((8, 128), F32),
                pltpu.VMEM((16, 8, 128), F32),
                pltpu.VMEM((16, 8, 128), F32),
                dma((16,)), dma((SLOTS,)), dma((4,)), dma((4,)), dma((2,)), dma((2,)), dma((2,)), dma((2,)),
                dma, dma, dma, dma, dma((10,)), dma((10,)), dma((groups,)), dma((groups,)), dma, dma,
                dma((16,)), dma((16,)), dma((16,)), dma((16,)),
            ],
            compiler_params=pltpu.CompilerParams(vmem_limit_bytes=67043328, has_side_effects=True, collective_id=0),
        )(pers_piece, restart_wt, adj_tile)
        return auth.transpose(0, 2, 1).reshape(chunk, dim), hub.T

    return jax.shard_map(
        device_fn, mesh=mesh,
        in_specs=(P("row", "col"), P(("row", "col"), None), P(None, None)),
        out_specs=(P(("col", "row"), None), P(("row", "col"), None)), check_vma=False)
```

```python
import functools

import jax
import jax.numpy as jnp
from jax import lax
from jax.experimental import pallas as pl
from jax.experimental.pallas import tpu as pltpu
from jax.sharding import PartitionSpec as P

F32, BF16 = jnp.float32, jnp.bfloat16
MESH = pl.DeviceIdType.MESH
SLOTS = 6


def prod_cols(lhs, rhs):
    return lax.dot_general(lhs, rhs, (((1,), (0,)), ((), ())), preferred_element_type=F32)


def prod_rows(lhs, rhs, zero):
    cols = []
    size_m, size_n = min(256, rhs.shape[0]), min(256, rhs.shape[1])
    for r in range(0, rhs.shape[0], size_m):
        val = None
        for c in range(0, rhs.shape[1], size_n):
            tile = rhs[r:r + size_m, c:c + size_n].T
            tile = tile + jnp.tile(zero, (tile.shape[0] // zero.shape[0], tile.shape[1] // zero.shape[1]))
            part = prod_cols(lhs[:, c:c + size_n], tile)
            val = part if val is None else val + part
        cols.append(val)
    return jnp.concatenate(cols, axis=1)


def lane_tile(v, width):
    return jnp.concatenate([v] * (width // 128), axis=1)


def row_to_lanes(row, dim):
    return jnp.broadcast_to(row, (128, 128)).T[:dim]


def square_sums(parts):
    total = None
    for part in parts:
        for t in range(part.shape[1] // 128):
            v = part[:, t * 128:(t + 1) * 128]
            total = v * v if total is None else total + v * v
    full = jnp.concatenate([total, jnp.zeros((128 - total.shape[0], 128), F32)], axis=0)
    row = jnp.sum(full.T, axis=0, keepdims=True)
    return jnp.broadcast_to(row, (8, 128))


def kernel(n_total, v_ref, b_ref, a_hbm, auth_out, hub_out,
           res, stm, vt, bt, hb, ab, acc, own_sum, oth_sum, rd, s1x, s1y, s2x, s2y, zr, none_ref, sq_send, sq1, sq2,
           res_sem, stm_sem, dd_s, dd_r, x1_s, x1_r, y1_s, y1_r, x2_s, x2_r, y2_s, y2_r,
           ag_s, ag_r, z_s, z_r, h_s, h_r, q1_s, q1_r, q2_s, q2_r):
    sweeps, dim = b_ref.shape
    rows, width = stm.shape[1], stm.shape[2]
    groups, span = oth_sum.shape[0], oth_sum.shape[2]
    j, i = lax.axis_index("col"), lax.axis_index("row")
    core, x, y = i % 2, (i // 2) % 2, i // 4
    partner = {"row": i + 1 - 2 * core, "col": j}
    xnb = {"row": i + 2 - 4 * x, "col": j}
    ynb = {"row": i + 4 - 8 * y, "col": j}
    znb = {"row": i, "col": 1 - j}
    base_o, base_x = 4 * y + 2 * x, 4 * y + 2 * (1 - x)
    base_y, base_d = 4 * (1 - y) + 2 * x, 4 * (1 - y) + 2 * (1 - x)
    mine, other = core, 1 - core
    ord1 = [base_d + other, base_d + mine, base_x + other, base_x + mine,
            base_y + other, base_y + mine, base_o + mine, base_o + other]
    ord2 = [base_o + mine, base_o + other, base_x + mine, base_y + mine,
            base_x + other, base_y + other, base_d + other, base_d + mine]

    def rcopy(src, dst, s, r, dev):
        return pltpu.make_async_remote_copy(src, dst, s, r, device_id=dev, device_id_type=MESH)

    def a_block(which, chunk, half):
        return a_hbm.at[pl.ds(pl.multiple_of(which * rows, rows), rows),
                        pl.ds(pl.multiple_of((chunk * 2 + half) * width, width), width)]

    def load(chunk, half, slot, own):
        return pltpu.make_async_copy(a_block(j if own else 1 - j, chunk, half), stm.at[slot], stm_sem.at[slot])

    def load_res(q, half, own):
        return pltpu.make_async_copy(a_block(j if own else 1 - j, ord1[q], half), res.at[ord1[q], half],
                                     res_sem.at[2 * q + half])

    def block_wait(ci, order, far):
        slots = [(2 * ci + half) % SLOTS for half in range(2)]
        if ci >= 2:
            for half in range(2):
                load(order[ci], half, slots[half], ci in far).wait()
        return slots

    def block_next(ci, order, after, far, half=None):
        for h in range(2) if half is None else (half,):
            slot = (2 * ci + h) % SLOTS
            if ci <= 4:
                load(order[ci + 3], h, slot, ci + 3 in far).start()
            elif ci == 5:
                load(after[2], h, slot, False).start()

    def copies_h():
        return [rcopy(hb.at[0, part], hb.at[1, part], h_s.at[part], h_r.at[part], znb) for part in range(2)]

    def send_h(val):
        for part in range(2):
            hb[0, part] = val[:, part * width:(part + 1) * width].astype(BF16)
        for c in copies_h():
            c.start()

    def cols_of(which, blocks, part=None):
        val = None
        for q in range(2) if part is None else (part,):
            p = prod_cols(hb[which, q], blocks[q * width:(q + 1) * width, :])
            val = p if val is None else val + p
        return val

    def own_near():
        def pair(t, c):
            for base in (base_x, base_y):
                for half in range(2):
                    acc[base + t, half] = cols_of(0, res[base + t, half])
            return c
        lax.fori_loop(0, 2, pair, 0)

    def all_sum(row8, buf, send, recv):
        sq_send[...] = row8
        buf[0] = row8
        copies = []
        for d in range(15, 0, -1):
            dz, dy, dx, dc = d // 8, (d // 4) % 2, (d // 2) % 2, d % 2
            dev = {"row": 4 * ((y + dy) % 2) + 2 * ((x + dx) % 2) + (core + dc) % 2, "col": (j + dz) % 2}
            copies.append(rcopy(sq_send, buf.at[d], send.at[d], recv.at[d], dev))
            copies[-1].start()
        for c in copies:
            c.wait_recv()
        vals = [buf[d] for d in range(16)]
        while len(vals) > 1:
            vals = [vals[q] + vals[q + 1] for q in range(0, len(vals), 2)]
        scale = lax.rsqrt(vals[0] / n_total)
        cols = row_to_lanes(scale[:1], dim)
        for c in copies:
            c.wait_send()
        return cols

    none_ref[...] = jnp.zeros(none_ref.shape, BF16)
    for u in range(4):
        load(ord1[u // 2], u % 2, u, True).start()
    for q in (2, 3, 4, 5, 0, 1):
        for half in range(2):
            load_res(q, half, q >= 2).start()
    for half in range(2):
        load(ord1[2], half, 4 + half, False).start()
    for q in (6, 7):
        for half in range(2):
            load_res(q, half, True).start()
    barrier = pltpu.get_barrier_semaphore()
    for d in range(1, 16):
        dz, dy, dx, dc = d // 8, (d // 4) % 2, (d // 2) % 2, d % 2
        dev = {"row": 4 * ((y + dy) % 2) + 2 * ((x + dx) % 2) + (core + dc) % 2, "col": (j + dz) % 2}
        pl.semaphore_signal(barrier, inc=1, device_id=dev, device_id_type=MESH)
    pad = jnp.zeros((128, 128 - dim), F32)
    for t in range(rows // 128):
        tile = jnp.concatenate([v_ref[t * 128:(t + 1) * 128, :], pad], axis=1)
        vt[:, t * 128:(t + 1) * 128] = tile.T[:dim]
    pl.semaphore_wait(barrier, 15)
    send_h(vt[...])
    for k in range(sweeps):
        bt[k] = row_to_lanes(jnp.concatenate([b_ref[k:k + 1, :], pad[:1]], axis=1), dim)

    for q in range(2):
        for half in range(2):
            load(ord1[q], half, 2 * q + half, True).wait()
    far1, far2 = (0, 1), (6, 7)

    def own_far():
        for q in range(2):
            for half in range(2):
                acc[ord1[q], half] = cols_of(0, stm[2 * q + half])
        for q in range(2):
            block_next(q, ord1, ord2, far1)

    own_far()
    for q in range(2, 6):
        for half in range(2):
            load_res(q, half, True).wait()
    own_near()
    for q in (0, 1, 6, 7):
        for half in range(2):
            load_res(q, half, q >= 6).wait()

    def sweep(k, carry):
        with jax.named_scope("hwait"):
            h_cps = copies_h()
            h_cps[0].wait_recv()
        with jax.named_scope("d0"):
            for q in range(2):
                for half in range(2):
                    acc[ord1[q], half] += cols_of(1, res[ord1[q], half], 0)
        with jax.named_scope("hwait2"):
            h_cps[1].wait_recv()
        d_mine, x_mine, y_mine, o_mine = ord1[1], ord1[3], ord1[5], ord1[6]
        gives = [ord1[0], ord1[2], ord1[4], ord1[7]]
        keeps = [d_mine, x_mine, y_mine, o_mine]
        dd = [rcopy(acc.at[gives[t]], rd.at[t], dd_s.at[t], dd_r.at[t], partner) for t in range(4)]
        x1 = [rcopy(acc.at[d_mine, 0], s1x.at[0], x1_s.at[0], x1_r.at[0], xnb),
              rcopy(acc.at[x_mine, 0], s1x.at[1], x1_s.at[1], x1_r.at[1], xnb)]
        y1 = [rcopy(acc.at[d_mine, 1], s1y.at[0], y1_s.at[0], y1_r.at[0], ynb),
              rcopy(acc.at[y_mine, 1], s1y.at[1], y1_s.at[1], y1_r.at[1], ynb)]
        x2 = rcopy(acc.at[x_mine, 1], s2x, x2_s, x2_r, xnb)
        y2 = rcopy(acc.at[y_mine, 0], s2y, y2_s, y2_r, ynb)

        def far_rows(ci):
            for half in range(2):
                acc[ord1[ci], half] += cols_of(1, res[ord1[ci], half], 1)

        def other_rows(ci):
            chunk = ord1[ci]
            slots = block_wait(ci, ord1, far1)
            for half in range(2):
                val = cols_of(1, stm[slots[half]])
                if ci >= 6:
                    acc[chunk, half] = cols_of(0, res[chunk, half]) + val
                else:
                    acc[chunk, half] += val
            block_next(ci, ord1, ord2, far1)

        def combine(t):
            dd[t].wait_recv()
            acc[keeps[t]] += rd[t]

        with jax.named_scope("p1a"):
            far_rows(0)
            dd[0].start()
            far_rows(1)
            other_rows(2)
            dd[1].start()
        with jax.named_scope("comb0"):
            combine(0)
            x1[0].start()
            y1[0].start()
        with jax.named_scope("p1b"):
            other_rows(3)
            other_rows(4)
            dd[2].start()
        with jax.named_scope("comb1"):
            combine(1)
            x1[1].start()
        with jax.named_scope("p1c"):
            other_rows(5)
        with jax.named_scope("comb2"):
            combine(2)
            y1[1].start()
        with jax.named_scope("p1d"):
            other_rows(6)
            other_rows(7)
            dd[3].start()
        with jax.named_scope("rs2"):
            x1[0].wait_recv()
            acc[y_mine, 0] += s1x[0]
            y2.start()
            y1[0].wait_recv()
            acc[x_mine, 1] += s1y[0]
            x2.start()
        with jax.named_scope("rs3"):
            combine(3)
            x1[1].wait_recv()
            y1[1].wait_recv()
            p0 = acc[o_mine, 0] + s1x[1]
            p1 = acc[o_mine, 1] + s1y[1]
            acc[o_mine, 0] = p0
            acc[o_mine, 1] = p1
        with jax.named_scope("rs4"):
            y2.wait_recv()
            x2.wait_recv()
            p0 = acc[o_mine, 0] + s2y[...]
            p1 = acc[o_mine, 1] + s2x[...]
            auth_out[0] = p0
            auth_out[1] = p1
        with jax.named_scope("ar1"):
            scale = all_sum(square_sums([p0, p1]), sq1, q1_s, q1_r)
        with jax.named_scope("norm1"):
            wide = lane_tile(scale, width)
            for half in range(2):
                val = auth_out[half] * wide
                auth_out[half] = val
                ab[i, half] = val.astype(BF16)
            for c in dd + x1 + y1 + [x2, y2, *h_cps]:
                c.wait_send()

        px, py, pd = ord1[3], ord1[5], ord1[1]
        to_p = rcopy(ab.at[i], ab.at[i], ag_s.at[0], ag_r.at[0], partner)
        to_x = [rcopy(ab.at[i, h], ab.at[i, h], ag_s.at[1 + h], ag_r.at[1 + h], xnb) for h in range(2)]
        to_y = [rcopy(ab.at[i, h], ab.at[i, h], ag_s.at[3 + h], ag_r.at[3 + h], ynb) for h in range(2)]
        rel_y = rcopy(ab.at[px, 0], ab.at[px, 0], ag_s.at[5], ag_r.at[5], ynb)
        rel_x = rcopy(ab.at[py, 1], ab.at[py, 1], ag_s.at[6], ag_r.at[6], xnb)
        fw_x = rcopy(ab.at[px], ab.at[px], ag_s.at[7], ag_r.at[7], partner)
        fw_y = rcopy(ab.at[py], ab.at[py], ag_s.at[8], ag_r.at[8], partner)
        fw_d = rcopy(ab.at[pd], ab.at[pd], ag_s.at[9], ag_r.at[9], partner)
        to_p.start()
        to_x[0].start()
        to_y[1].start()
        to_x[1].start()
        to_y[0].start()

        zero = none_ref[...]

        def rows_of(chunk, half, block):
            return prod_rows(ab[chunk, half], block, zero)

        def resident(chunk):
            return rows_of(chunk, 0, res[chunk, 0]) + rows_of(chunk, 1, res[chunk, 1])

        def add_other(val, first=False):
            for g in range(groups):
                part = val[:, g * span:(g + 1) * span]
                if first:
                    oth_sum[g] = part
                else:
                    oth_sum[g] += part

        def streamed(ci, first=False):
            chunk = ord2[ci]
            slots = block_wait(ci, ord2, far2)
            add_other(rows_of(chunk, 0, stm[slots[0]]) + rows_of(chunk, 1, stm[slots[1]]), first)
            block_next(ci, ord2, ord1, far2)

        with jax.named_scope("p2a"):
            streamed(0, first=True)
        with jax.named_scope("pwait"):
            to_p.wait_recv()
        with jax.named_scope("p2b"):
            streamed(1)
            own_sum[...] = resident(ord2[0]) + resident(ord2[1])
        with jax.named_scope("xwait"):
            to_x[0].wait_recv()
            rel_y.start()
            to_y[1].wait_recv()
            rel_x.start()
        with jax.named_scope("p2c"):
            slots = block_wait(2, ord2, far2) + block_wait(3, ord2, far2)
            add_other(rows_of(ord2[2], 0, stm[slots[0]]) + rows_of(ord2[3], 1, stm[slots[3]]))
            block_next(2, ord2, ord1, far2, 0)
            block_next(3, ord2, ord1, far2, 1)
        with jax.named_scope("xwait2"):
            to_x[1].wait_recv()
            fw_x.start()
            to_y[0].wait_recv()
            fw_y.start()
        with jax.named_scope("p2d"):
            add_other(rows_of(ord2[2], 1, stm[slots[1]]) + rows_of(ord2[3], 0, stm[slots[2]]))
            block_next(2, ord2, ord1, far2, 1)
            block_next(3, ord2, ord1, far2, 0)
        with jax.named_scope("fxwait"):
            fw_x.wait_recv()
        with jax.named_scope("p2e"):
            streamed(4)
        with jax.named_scope("dwait"):
            rel_y.wait_recv()
            rel_x.wait_recv()
            fw_d.start()
            fw_y.wait_recv()
        with jax.named_scope("p2f"):
            streamed(5)
        with jax.named_scope("fdwait"):
            fw_d.wait_recv()
        with jax.named_scope("p2g"):
            z_cps = [rcopy(oth_sum.at[g], zr.at[g], z_s.at[g], z_r.at[g], znb) for g in range(groups)]
            for g in range(groups):
                val = oth_sum[g]
                for q in (6, 7):
                    for half in range(2):
                        val += rows_of(ord2[q], half, res[ord2[q], half, g * span:(g + 1) * span, :])
                oth_sum[g] = val
                z_cps[g].start()

        with jax.named_scope("p2rest"):
            def pair(t, c):
                own_sum[...] += resident(base_x + t) + resident(base_y + t)
                return c
            lax.fori_loop(0, 2, pair, 0)
            slots = block_wait(6, ord2, far2) + block_wait(7, ord2, far2)
            for q in range(4):
                own_sum[...] += rows_of(ord2[6 + q // 2], q % 2, stm[slots[q]])
        with jax.named_scope("zwait"):
            for g in range(groups):
                z_cps[g].wait_recv()
        with jax.named_scope("ar2"):
            val = own_sum[...] + jnp.concatenate([zr[g] for g in range(groups)], axis=1)
            own_sum[...] = val
            scale = all_sum(square_sums([val]), sq2, q2_s, q2_r)
        with jax.named_scope("upd"):
            wt = bt[k]
            hv = lane_tile(1.0 - wt, rows) * (own_sum[...] * lane_tile(scale, rows)) + lane_tile(wt, rows) * vt[...]
            hub_out[...] = hv
            for c in [to_p, *to_x, *to_y, rel_y, rel_x, fw_x, fw_y, fw_d, *z_cps]:
                c.wait_send()

        with jax.named_scope("own"):
            @pl.when(k < sweeps - 1)
            def _():
                send_h(hub_out[...])
                own_far()
                own_near()
        return carry

    lax.fori_loop(0, sweeps, sweep, 0)
    for half in range(2):
        load(ord1[2], half, 4 + half, False).wait()


def solution(mesh):
    def device_fn(adj_tile, pers_piece, restart_wt):
        sweeps, dim = restart_wt.shape
        chunk = pers_piece.shape[0]
        width = chunk // 2
        n_total = float(chunk * mesh.size)
        groups = 3 if chunk % 384 == 0 else 2
        vmem = pl.BlockSpec(memory_space=pltpu.VMEM)
        dma = pltpu.SemaphoreType.DMA
        auth, hub = pl.pallas_call(
            functools.partial(kernel, n_total),
            out_shape=(jax.ShapeDtypeStruct((2, dim, width), F32), jax.ShapeDtypeStruct((dim, chunk), F32)),
            in_specs=[vmem, vmem, pl.BlockSpec(memory_space=pl.ANY)],
            out_specs=(vmem, vmem),
            scratch_shapes=[
                pltpu.VMEM((8, 2, chunk, width), BF16),
                pltpu.VMEM((SLOTS, chunk, width), BF16),
                pltpu.VMEM((dim, chunk), F32),
                pltpu.VMEM((sweeps, dim, 128), F32),
                pltpu.VMEM((2, 2, dim, width), BF16),
                pltpu.VMEM((8, 2, dim, width), BF16),
                pltpu.VMEM((8, 2, dim, width), F32),
                pltpu.VMEM((dim, chunk), F32),
                pltpu.VMEM((groups, dim, chunk // groups), F32),
                pltpu.VMEM((4, 2, dim, width), F32),
                pltpu.VMEM((2, dim, width), F32),
                pltpu.VMEM((2, dim, width), F32),
                pltpu.VMEM((dim, width), F32),
                pltpu.VMEM((dim, width), F32),
                pltpu.VMEM((groups, dim, chunk // groups), F32),
                pltpu.VMEM((16, 128), BF16),
                pltpu.VMEM((8, 128), F32),
                pltpu.VMEM((16, 8, 128), F32),
                pltpu.VMEM((16, 8, 128), F32),
                dma((16,)), dma((SLOTS,)), dma((4,)), dma((4,)), dma((2,)), dma((2,)), dma((2,)), dma((2,)),
                dma, dma, dma, dma, dma((10,)), dma((10,)), dma((groups,)), dma((groups,)), dma((2,)), dma((2,)),
                dma((16,)), dma((16,)), dma((16,)), dma((16,)),
            ],
            compiler_params=pltpu.CompilerParams(vmem_limit_bytes=67043328, has_side_effects=True, collective_id=0),
        )(pers_piece, restart_wt, adj_tile)
        return auth.transpose(0, 2, 1).reshape(chunk, dim), hub.T

    return jax.shard_map(
        device_fn, mesh=mesh,
        in_specs=(P("row", "col"), P(("row", "col"), None), P(None, None)),
        out_specs=(P(("col", "row"), None), P(("row", "col"), None)), check_vma=False)
```

```python
import functools

import jax
import jax.numpy as jnp
from jax import lax
from jax.experimental import pallas as pl
from jax.experimental.pallas import tpu as pltpu
from jax.sharding import PartitionSpec as P

F32, BF16 = jnp.float32, jnp.bfloat16
MESH = pl.DeviceIdType.MESH
SLOTS = 6


def prod_cols(lhs, rhs):
    return lax.dot_general(lhs, rhs, (((1,), (0,)), ((), ())), preferred_element_type=F32)


def prod_rows(lhs, rhs, zero):
    cols = []
    size_m, size_n = min(256, rhs.shape[0]), min(256, rhs.shape[1])
    for r in range(0, rhs.shape[0], size_m):
        val = None
        for c in range(0, rhs.shape[1], size_n):
            tile = rhs[r:r + size_m, c:c + size_n]
            if (c // size_n) % 3 == 2:
                part = lax.dot_general(lhs[:, c:c + size_n], tile, (((1,), (1,)), ((), ())), preferred_element_type=F32)
            else:
                tile = tile.T
                tile = tile + jnp.tile(zero, (tile.shape[0] // zero.shape[0], tile.shape[1] // zero.shape[1]))
                part = prod_cols(lhs[:, c:c + size_n], tile)
            val = part if val is None else val + part
        cols.append(val)
    return jnp.concatenate(cols, axis=1)


def lane_tile(v, width):
    return jnp.concatenate([v] * (width // 128), axis=1)


def row_to_lanes(row, dim):
    return jnp.broadcast_to(row, (128, 128)).T[:dim]


def square_sums(parts):
    total = None
    for part in parts:
        for t in range(part.shape[1] // 128):
            v = part[:, t * 128:(t + 1) * 128]
            total = v * v if total is None else total + v * v
    full = jnp.concatenate([total, jnp.zeros((128 - total.shape[0], 128), F32)], axis=0)
    row = jnp.sum(full.T, axis=0, keepdims=True)
    return jnp.broadcast_to(row, (8, 128))


def kernel(n_total, v_ref, b_ref, a_hbm, auth_out, hub_out,
           res, stm, vt, bt, hb, ab, acc, own_sum, oth_sum, rd, s1x, s1y, s2x, s2y, zr, none_ref, sq_send, sq1, sq2,
           res_sem, stm_sem, dd_s, dd_r, x1_s, x1_r, y1_s, y1_r, x2_s, x2_r, y2_s, y2_r,
           ag_s, ag_r, z_s, z_r, h_s, h_r, q1_s, q1_r, q2_s, q2_r):
    sweeps, dim = b_ref.shape
    rows, width = stm.shape[1], stm.shape[2]
    groups, span = oth_sum.shape[0], oth_sum.shape[2]
    j, i = lax.axis_index("col"), lax.axis_index("row")
    core, x, y = i % 2, (i // 2) % 2, i // 4
    partner = {"row": i + 1 - 2 * core, "col": j}
    xnb = {"row": i + 2 - 4 * x, "col": j}
    ynb = {"row": i + 4 - 8 * y, "col": j}
    znb = {"row": i, "col": 1 - j}
    base_o, base_x = 4 * y + 2 * x, 4 * y + 2 * (1 - x)
    base_y, base_d = 4 * (1 - y) + 2 * x, 4 * (1 - y) + 2 * (1 - x)
    mine, other = core, 1 - core
    ord1 = [base_d + other, base_d + mine, base_x + other, base_x + mine,
            base_y + other, base_y + mine, base_o + mine, base_o + other]
    ord2 = [base_o + mine, base_o + other, base_x + mine, base_y + mine,
            base_x + other, base_y + other, base_d + other, base_d + mine]

    def rcopy(src, dst, s, r, dev):
        return pltpu.make_async_remote_copy(src, dst, s, r, device_id=dev, device_id_type=MESH)

    def a_block(which, chunk, half):
        return a_hbm.at[pl.ds(pl.multiple_of(which * rows, rows), rows),
                        pl.ds(pl.multiple_of((chunk * 2 + half) * width, width), width)]

    def load(chunk, half, slot, own):
        return pltpu.make_async_copy(a_block(j if own else 1 - j, chunk, half), stm.at[slot], stm_sem.at[slot])

    def load_res(q, half, own):
        return pltpu.make_async_copy(a_block(j if own else 1 - j, ord1[q], half), res.at[ord1[q], half],
                                     res_sem.at[2 * q + half])

    def block_wait(ci, order, far):
        slots = [(2 * ci + half) % SLOTS for half in range(2)]
        if ci >= 2:
            for half in range(2):
                load(order[ci], half, slots[half], ci in far).wait()
        return slots

    def block_next(ci, order, after, far, half=None):
        for h in range(2) if half is None else (half,):
            slot = (2 * ci + h) % SLOTS
            if ci <= 4:
                load(order[ci + 3], h, slot, ci + 3 in far).start()
            elif ci == 5:
                load(after[2], h, slot, False).start()

    def copies_h():
        return [rcopy(hb.at[0, part], hb.at[1, part], h_s.at[part], h_r.at[part], znb) for part in range(2)]

    def send_h(val):
        for part in range(2):
            hb[0, part] = val[:, part * width:(part + 1) * width].astype(BF16)
        for c in copies_h():
            c.start()

    def cols_of(which, blocks):
        return prod_cols(jnp.concatenate([hb[which, 0], hb[which, 1]], axis=1), blocks)

    def own_near():
        def pair(t, c):
            for base in (base_x, base_y):
                for half in range(2):
                    acc[base + t, half] = cols_of(0, res[base + t, half])
            return c
        lax.fori_loop(0, 2, pair, 0)

    def all_sum(row8, buf, send, recv):
        sq_send[...] = row8
        buf[0] = row8
        copies = []
        for d in range(15, 0, -1):
            dz, dy, dx, dc = d // 8, (d // 4) % 2, (d // 2) % 2, d % 2
            dev = {"row": 4 * ((y + dy) % 2) + 2 * ((x + dx) % 2) + (core + dc) % 2, "col": (j + dz) % 2}
            copies.append(rcopy(sq_send, buf.at[d], send.at[d], recv.at[d], dev))
            copies[-1].start()
        for c in copies:
            c.wait_recv()
        vals = [buf[d] for d in range(16)]
        while len(vals) > 1:
            vals = [vals[q] + vals[q + 1] for q in range(0, len(vals), 2)]
        scale = lax.rsqrt(vals[0] / n_total)
        cols = row_to_lanes(scale[:1], dim)
        for c in copies:
            c.wait_send()
        return cols

    none_ref[...] = jnp.zeros(none_ref.shape, BF16)
    for u in range(4):
        load(ord1[u // 2], u % 2, u, True).start()
    for q in (2, 3, 4, 5, 0, 1):
        for half in range(2):
            load_res(q, half, q >= 2).start()
    for half in range(2):
        load(ord1[2], half, 4 + half, False).start()
    for q in (6, 7):
        for half in range(2):
            load_res(q, half, True).start()
    barrier = pltpu.get_barrier_semaphore()
    for d in range(1, 16):
        dz, dy, dx, dc = d // 8, (d // 4) % 2, (d // 2) % 2, d % 2
        dev = {"row": 4 * ((y + dy) % 2) + 2 * ((x + dx) % 2) + (core + dc) % 2, "col": (j + dz) % 2}
        pl.semaphore_signal(barrier, inc=1, device_id=dev, device_id_type=MESH)
    pad = jnp.zeros((128, 128 - dim), F32)
    for t in range(rows // 128):
        tile = jnp.concatenate([v_ref[t * 128:(t + 1) * 128, :], pad], axis=1)
        vt[:, t * 128:(t + 1) * 128] = tile.T[:dim]
    pl.semaphore_wait(barrier, 15)
    send_h(vt[...])
    for k in range(sweeps):
        bt[k] = row_to_lanes(jnp.concatenate([b_ref[k:k + 1, :], pad[:1]], axis=1), dim)

    for q in range(2):
        for half in range(2):
            load(ord1[q], half, 2 * q + half, True).wait()
    far1, far2 = (0, 1), (6, 7)

    def own_far():
        for q in range(2):
            for half in range(2):
                acc[ord1[q], half] = cols_of(0, stm[2 * q + half])
        for q in range(2):
            block_next(q, ord1, ord2, far1)

    own_far()
    for q in range(2, 6):
        for half in range(2):
            load_res(q, half, True).wait()
    own_near()
    for q in (0, 1, 6, 7):
        for half in range(2):
            load_res(q, half, q >= 6).wait()

    def sweep(k, carry):
        with jax.named_scope("hwait"):
            h_cps = copies_h()
            h_cps[0].wait_recv()
        h_cps[1].wait_recv()
        d_mine, x_mine, y_mine, o_mine = ord1[1], ord1[3], ord1[5], ord1[6]
        gives = [ord1[0], ord1[2], ord1[4], ord1[7]]
        keeps = [d_mine, x_mine, y_mine, o_mine]
        dd = [rcopy(acc.at[gives[t]], rd.at[t], dd_s.at[t], dd_r.at[t], partner) for t in range(4)]
        x1 = [rcopy(acc.at[d_mine, 0], s1x.at[0], x1_s.at[0], x1_r.at[0], xnb),
              rcopy(acc.at[x_mine, 0], s1x.at[1], x1_s.at[1], x1_r.at[1], xnb)]
        y1 = [rcopy(acc.at[d_mine, 1], s1y.at[0], y1_s.at[0], y1_r.at[0], ynb),
              rcopy(acc.at[y_mine, 1], s1y.at[1], y1_s.at[1], y1_r.at[1], ynb)]
        x2 = rcopy(acc.at[x_mine, 1], s2x, x2_s, x2_r, xnb)
        y2 = rcopy(acc.at[y_mine, 0], s2y, y2_s, y2_r, ynb)

        def far_rows(ci):
            for half in range(2):
                acc[ord1[ci], half] += cols_of(1, res[ord1[ci], half])

        def other_rows(ci):
            chunk = ord1[ci]
            slots = block_wait(ci, ord1, far1)
            for half in range(2):
                val = cols_of(1, stm[slots[half]])
                if ci >= 6:
                    acc[chunk, half] = cols_of(0, res[chunk, half]) + val
                else:
                    acc[chunk, half] += val
            block_next(ci, ord1, ord2, far1)

        def combine(t):
            dd[t].wait_recv()
            acc[keeps[t]] += rd[t]

        with jax.named_scope("p1a"):
            far_rows(0)
            dd[0].start()
            far_rows(1)
            other_rows(2)
            dd[1].start()
        with jax.named_scope("comb0"):
            combine(0)
            x1[0].start()
            y1[0].start()
        with jax.named_scope("p1b"):
            other_rows(3)
            other_rows(4)
            dd[2].start()
        with jax.named_scope("comb1"):
            combine(1)
            x1[1].start()
        with jax.named_scope("p1c"):
            other_rows(5)
        with jax.named_scope("comb2"):
            combine(2)
            y1[1].start()
        with jax.named_scope("p1d"):
            other_rows(6)
            other_rows(7)
            dd[3].start()
        with jax.named_scope("rs2"):
            x1[0].wait_recv()
            acc[y_mine, 0] += s1x[0]
            y2.start()
            y1[0].wait_recv()
            acc[x_mine, 1] += s1y[0]
            x2.start()
        with jax.named_scope("rs3"):
            combine(3)
            x1[1].wait_recv()
            y1[1].wait_recv()
            p0 = acc[o_mine, 0] + s1x[1]
            p1 = acc[o_mine, 1] + s1y[1]
            acc[o_mine, 0] = p0
            acc[o_mine, 1] = p1
        with jax.named_scope("rs4"):
            y2.wait_recv()
            x2.wait_recv()
            p0 = acc[o_mine, 0] + s2y[...]
            p1 = acc[o_mine, 1] + s2x[...]
            auth_out[0] = p0
            auth_out[1] = p1
        with jax.named_scope("ar1"):
            scale = all_sum(square_sums([p0, p1]), sq1, q1_s, q1_r)
        with jax.named_scope("norm1"):
            wide = lane_tile(scale, width)
            for half in range(2):
                val = auth_out[half] * wide
                auth_out[half] = val
                ab[i, half] = val.astype(BF16)
            for c in dd + x1 + y1 + [x2, y2, *h_cps]:
                c.wait_send()

        px, py, pd = ord1[3], ord1[5], ord1[1]
        to_p = rcopy(ab.at[i], ab.at[i], ag_s.at[0], ag_r.at[0], partner)
        to_x = [rcopy(ab.at[i, h], ab.at[i, h], ag_s.at[1 + h], ag_r.at[1 + h], xnb) for h in range(2)]
        to_y = [rcopy(ab.at[i, h], ab.at[i, h], ag_s.at[3 + h], ag_r.at[3 + h], ynb) for h in range(2)]
        rel_y = rcopy(ab.at[px, 0], ab.at[px, 0], ag_s.at[5], ag_r.at[5], ynb)
        rel_x = rcopy(ab.at[py, 1], ab.at[py, 1], ag_s.at[6], ag_r.at[6], xnb)
        fw_x = rcopy(ab.at[px], ab.at[px], ag_s.at[7], ag_r.at[7], partner)
        fw_y = rcopy(ab.at[py], ab.at[py], ag_s.at[8], ag_r.at[8], partner)
        fw_d = rcopy(ab.at[pd], ab.at[pd], ag_s.at[9], ag_r.at[9], partner)
        to_p.start()
        to_x[0].start()
        to_y[1].start()
        to_x[1].start()
        to_y[0].start()

        zero = none_ref[...]

        def rows_of(chunk, half, block):
            return prod_rows(ab[chunk, half], block, zero)

        def resident(chunk):
            return rows_of(chunk, 0, res[chunk, 0]) + rows_of(chunk, 1, res[chunk, 1])

        def add_other(val, first=False):
            for g in range(groups):
                part = val[:, g * span:(g + 1) * span]
                if first:
                    oth_sum[g] = part
                else:
                    oth_sum[g] += part

        def streamed(ci, first=False):
            chunk = ord2[ci]
            slots = block_wait(ci, ord2, far2)
            add_other(rows_of(chunk, 0, stm[slots[0]]) + rows_of(chunk, 1, stm[slots[1]]), first)
            block_next(ci, ord2, ord1, far2)

        with jax.named_scope("p2a"):
            streamed(0, first=True)
        with jax.named_scope("pwait"):
            to_p.wait_recv()
        with jax.named_scope("p2b"):
            streamed(1)
            own_sum[...] = resident(ord2[0]) + resident(ord2[1])
        with jax.named_scope("xwait"):
            to_x[0].wait_recv()
            rel_y.start()
            to_y[1].wait_recv()
            rel_x.start()
        with jax.named_scope("p2c"):
            slots = block_wait(2, ord2, far2) + block_wait(3, ord2, far2)
            add_other(rows_of(ord2[2], 0, stm[slots[0]]) + rows_of(ord2[3], 1, stm[slots[3]]))
            block_next(2, ord2, ord1, far2, 0)
            block_next(3, ord2, ord1, far2, 1)
        with jax.named_scope("xwait2"):
            to_x[1].wait_recv()
            fw_x.start()
            to_y[0].wait_recv()
            fw_y.start()
        with jax.named_scope("p2d"):
            add_other(rows_of(ord2[2], 1, stm[slots[1]]) + rows_of(ord2[3], 0, stm[slots[2]]))
            block_next(2, ord2, ord1, far2, 1)
            block_next(3, ord2, ord1, far2, 0)
        with jax.named_scope("fxwait"):
            fw_x.wait_recv()
        with jax.named_scope("p2e"):
            streamed(4)
        with jax.named_scope("dwait"):
            rel_y.wait_recv()
            rel_x.wait_recv()
            fw_d.start()
            fw_y.wait_recv()
        with jax.named_scope("p2f"):
            streamed(5)
        with jax.named_scope("fdwait"):
            fw_d.wait_recv()
        with jax.named_scope("p2g"):
            z_cps = [rcopy(oth_sum.at[g], zr.at[g], z_s.at[g], z_r.at[g], znb) for g in range(groups)]
            for g in range(groups):
                val = oth_sum[g]
                for q in (6, 7):
                    for half in range(2):
                        val += rows_of(ord2[q], half, res[ord2[q], half, g * span:(g + 1) * span, :])
                oth_sum[g] = val
                z_cps[g].start()

        with jax.named_scope("p2rest"):
            def pair(t, c):
                own_sum[...] += resident(base_x + t) + resident(base_y + t)
                return c
            lax.fori_loop(0, 2, pair, 0)
            slots = block_wait(6, ord2, far2) + block_wait(7, ord2, far2)
            for q in range(4):
                own_sum[...] += rows_of(ord2[6 + q // 2], q % 2, stm[slots[q]])
        with jax.named_scope("zwait"):
            for g in range(groups):
                z_cps[g].wait_recv()
        with jax.named_scope("ar2"):
            val = own_sum[...] + jnp.concatenate([zr[g] for g in range(groups)], axis=1)
            own_sum[...] = val
            scale = all_sum(square_sums([val]), sq2, q2_s, q2_r)
        with jax.named_scope("upd"):
            wt = bt[k]
            hv = lane_tile(1.0 - wt, rows) * (own_sum[...] * lane_tile(scale, rows)) + lane_tile(wt, rows) * vt[...]
            hub_out[...] = hv
            for c in [to_p, *to_x, *to_y, rel_y, rel_x, fw_x, fw_y, fw_d, *z_cps]:
                c.wait_send()

        with jax.named_scope("own"):
            @pl.when(k < sweeps - 1)
            def _():
                send_h(hub_out[...])
                own_far()
                own_near()
        return carry

    lax.fori_loop(0, sweeps, sweep, 0)
    for half in range(2):
        load(ord1[2], half, 4 + half, False).wait()


def solution(mesh):
    def device_fn(adj_tile, pers_piece, restart_wt):
        sweeps, dim = restart_wt.shape
        chunk = pers_piece.shape[0]
        width = chunk // 2
        n_total = float(chunk * mesh.size)
        groups = 3 if chunk % 384 == 0 else 2
        vmem = pl.BlockSpec(memory_space=pltpu.VMEM)
        dma = pltpu.SemaphoreType.DMA
        auth, hub = pl.pallas_call(
            functools.partial(kernel, n_total),
            out_shape=(jax.ShapeDtypeStruct((2, dim, width), F32), jax.ShapeDtypeStruct((dim, chunk), F32)),
            in_specs=[vmem, vmem, pl.BlockSpec(memory_space=pl.ANY)],
            out_specs=(vmem, vmem),
            scratch_shapes=[
                pltpu.VMEM((8, 2, chunk, width), BF16),
                pltpu.VMEM((SLOTS, chunk, width), BF16),
                pltpu.VMEM((dim, chunk), F32),
                pltpu.VMEM((sweeps, dim, 128), F32),
                pltpu.VMEM((2, 2, dim, width), BF16),
                pltpu.VMEM((8, 2, dim, width), BF16),
                pltpu.VMEM((8, 2, dim, width), F32),
                pltpu.VMEM((dim, chunk), F32),
                pltpu.VMEM((groups, dim, chunk // groups), F32),
                pltpu.VMEM((4, 2, dim, width), F32),
                pltpu.VMEM((2, dim, width), F32),
                pltpu.VMEM((2, dim, width), F32),
                pltpu.VMEM((dim, width), F32),
                pltpu.VMEM((dim, width), F32),
                pltpu.VMEM((groups, dim, chunk // groups), F32),
                pltpu.VMEM((16, 128), BF16),
                pltpu.VMEM((8, 128), F32),
                pltpu.VMEM((16, 8, 128), F32),
                pltpu.VMEM((16, 8, 128), F32),
                dma((16,)), dma((SLOTS,)), dma((4,)), dma((4,)), dma((2,)), dma((2,)), dma((2,)), dma((2,)),
                dma, dma, dma, dma, dma((10,)), dma((10,)), dma((groups,)), dma((groups,)), dma((2,)), dma((2,)),
                dma((16,)), dma((16,)), dma((16,)), dma((16,)),
            ],
            compiler_params=pltpu.CompilerParams(vmem_limit_bytes=67043328, has_side_effects=True, collective_id=0),
        )(pers_piece, restart_wt, adj_tile)
        return auth.transpose(0, 2, 1).reshape(chunk, dim), hub.T

    return jax.shard_map(
        device_fn, mesh=mesh,
        in_specs=(P("row", "col"), P(("row", "col"), None), P(None, None)),
        out_specs=(P(("col", "row"), None), P(("row", "col"), None)), check_vma=False)
```

```python
import functools

import jax
import jax.numpy as jnp
from jax import lax
from jax.experimental import pallas as pl
from jax.experimental.pallas import tpu as pltpu
from jax.sharding import PartitionSpec as P

F32, BF16 = jnp.float32, jnp.bfloat16
MESH = pl.DeviceIdType.MESH
SLOTS = 6


def prod_cols(lhs, rhs):
    return lax.dot_general(lhs, rhs, (((1,), (0,)), ((), ())), preferred_element_type=F32)


def prod_rows(lhs, rhs, zero):
    cols = []
    size_m, size_n = min(256, rhs.shape[0]), min(256, rhs.shape[1])
    for r in range(0, rhs.shape[0], size_m):
        val = None
        for c in range(0, rhs.shape[1], size_n):
            tile = rhs[r:r + size_m, c:c + size_n]
            if (c // size_n) % 3 == 2:
                part = lax.dot_general(lhs[:, c:c + size_n], tile, (((1,), (1,)), ((), ())), preferred_element_type=F32)
            else:
                tile = tile.T
                tile = tile + jnp.tile(zero, (tile.shape[0] // zero.shape[0], tile.shape[1] // zero.shape[1]))
                part = prod_cols(lhs[:, c:c + size_n], tile)
            val = part if val is None else val + part
        cols.append(val)
    return jnp.concatenate(cols, axis=1)


def lane_tile(v, width):
    return jnp.concatenate([v] * (width // 128), axis=1)


def row_to_lanes(row, dim):
    return jnp.broadcast_to(row, (128, 128)).T[:dim]


def square_sums(parts):
    total = None
    for part in parts:
        for t in range(part.shape[1] // 128):
            v = part[:, t * 128:(t + 1) * 128]
            total = v * v if total is None else total + v * v
    full = jnp.concatenate([total, jnp.zeros((128 - total.shape[0], 128), F32)], axis=0)
    row = jnp.sum(full.T, axis=0, keepdims=True)
    return jnp.broadcast_to(row, (8, 128))


def kernel(n_total, v_ref, b_ref, a_hbm, auth_out, hub_out,
           res, stm, vt, bt, hb, ab, acc, own_sum, oth_sum, rd, s1x, s1y, s2x, s2y, zr, none_ref, sq_send, sq1, sq2,
           res_sem, stm_sem, dd_s, dd_r, x1_s, x1_r, y1_s, y1_r, x2_s, x2_r, y2_s, y2_r,
           ag_s, ag_r, z_s, z_r, h_s, h_r, q1_s, q1_r, q2_s, q2_r):
    sweeps, dim = b_ref.shape
    rows, width = stm.shape[1], stm.shape[2]
    groups, span = oth_sum.shape[0], oth_sum.shape[2]
    j, i = lax.axis_index("col"), lax.axis_index("row")
    core, x, y = i % 2, (i // 2) % 2, i // 4
    partner = {"row": i + 1 - 2 * core, "col": j}
    xnb = {"row": i + 2 - 4 * x, "col": j}
    ynb = {"row": i + 4 - 8 * y, "col": j}
    znb = {"row": i, "col": 1 - j}
    base_o, base_x = 4 * y + 2 * x, 4 * y + 2 * (1 - x)
    base_y, base_d = 4 * (1 - y) + 2 * x, 4 * (1 - y) + 2 * (1 - x)
    mine, other = core, 1 - core
    ord1 = [base_d + other, base_d + mine, base_x + other, base_x + mine,
            base_y + other, base_y + mine, base_o + mine, base_o + other]
    ord2 = [base_o + mine, base_o + other, base_x + mine, base_y + mine,
            base_x + other, base_y + other, base_d + other, base_d + mine]

    def rcopy(src, dst, s, r, dev):
        return pltpu.make_async_remote_copy(src, dst, s, r, device_id=dev, device_id_type=MESH)

    def a_block(which, chunk, half):
        return a_hbm.at[pl.ds(pl.multiple_of(which * rows, rows), rows),
                        pl.ds(pl.multiple_of((chunk * 2 + half) * width, width), width)]

    def load(chunk, half, slot, own):
        return pltpu.make_async_copy(a_block(j if own else 1 - j, chunk, half), stm.at[slot], stm_sem.at[slot])

    def load_res(q, half, own):
        return pltpu.make_async_copy(a_block(j if own else 1 - j, ord1[q], half), res.at[ord1[q], half],
                                     res_sem.at[2 * q + half])

    def block_wait(ci, order, far):
        slots = [(2 * ci + half) % SLOTS for half in range(2)]
        if ci >= 2:
            for half in range(2):
                load(order[ci], half, slots[half], ci in far).wait()
        return slots

    def block_next(ci, order, after, far, half=None):
        for h in range(2) if half is None else (half,):
            slot = (2 * ci + h) % SLOTS
            if ci <= 4:
                load(order[ci + 3], h, slot, ci + 3 in far).start()
            elif ci == 5:
                load(after[2], h, slot, False).start()

    def copies_h():
        return [rcopy(hb.at[0, part], hb.at[1, part], h_s.at[part], h_r.at[part], znb) for part in range(2)]

    def send_h(val):
        for part in range(2):
            hb[0, part] = val[:, part * width:(part + 1) * width].astype(BF16)
        for c in copies_h():
            c.start()

    def cols_of(which, blocks):
        return prod_cols(jnp.concatenate([hb[which, 0], hb[which, 1]], axis=1), blocks)

    def own_near():
        def pair(t, c):
            for base in (base_x, base_y):
                for half in range(2):
                    acc[base + t, half] = cols_of(0, res[base + t, half])
            return c
        lax.fori_loop(0, 2, pair, 0)

    def all_sum(row8, buf, send, recv):
        sq_send[...] = row8
        buf[0] = row8
        copies = []
        for d in range(15, 0, -1):
            dz, dy, dx, dc = d // 8, (d // 4) % 2, (d // 2) % 2, d % 2
            dev = {"row": 4 * ((y + dy) % 2) + 2 * ((x + dx) % 2) + (core + dc) % 2, "col": (j + dz) % 2}
            copies.append(rcopy(sq_send, buf.at[d], send.at[d], recv.at[d], dev))
            copies[-1].start()
        for c in copies:
            c.wait_recv()
        vals = [buf[d] for d in range(16)]
        while len(vals) > 1:
            vals = [vals[q] + vals[q + 1] for q in range(0, len(vals), 2)]
        scale = lax.rsqrt(vals[0] / n_total)
        cols = row_to_lanes(scale[:1], dim)
        for c in copies:
            c.wait_send()
        return cols

    none_ref[...] = jnp.zeros(none_ref.shape, BF16)
    for u in range(4):
        load(ord1[u // 2], u % 2, u, True).start()
    for q in (2, 3, 4, 5, 0, 1):
        for half in range(2):
            load_res(q, half, q >= 2).start()
    for half in range(2):
        load(ord1[2], half, 4 + half, False).start()
    for q in (6, 7):
        for half in range(2):
            load_res(q, half, True).start()
    barrier = pltpu.get_barrier_semaphore()
    for d in range(1, 16):
        dz, dy, dx, dc = d // 8, (d // 4) % 2, (d // 2) % 2, d % 2
        dev = {"row": 4 * ((y + dy) % 2) + 2 * ((x + dx) % 2) + (core + dc) % 2, "col": (j + dz) % 2}
        pl.semaphore_signal(barrier, inc=1, device_id=dev, device_id_type=MESH)
    pad = jnp.zeros((128, 128 - dim), F32)
    for t in range(rows // 128):
        tile = jnp.concatenate([v_ref[t * 128:(t + 1) * 128, :], pad], axis=1)
        vt[:, t * 128:(t + 1) * 128] = tile.T[:dim]
    pl.semaphore_wait(barrier, 15)
    send_h(vt[...])
    for k in range(sweeps):
        bt[k] = row_to_lanes(jnp.concatenate([b_ref[k:k + 1, :], pad[:1]], axis=1), dim)

    for q in range(2):
        for half in range(2):
            load(ord1[q], half, 2 * q + half, True).wait()
    far1, far2 = (0, 1), (6, 7)

    def own_far():
        for q in range(2):
            for half in range(2):
                acc[ord1[q], half] = cols_of(0, stm[2 * q + half])
        for q in range(2):
            block_next(q, ord1, ord2, far1)

    own_far()
    for q in range(2, 6):
        for half in range(2):
            load_res(q, half, True).wait()
    own_near()
    for q in (0, 1, 6, 7):
        for half in range(2):
            load_res(q, half, q >= 6).wait()

    def sweep(k, carry):
        with jax.named_scope("hwait"):
            h_cps = copies_h()
            h_cps[0].wait_recv()
        h_cps[1].wait_recv()
        d_mine, x_mine, y_mine, o_mine = ord1[1], ord1[3], ord1[5], ord1[6]
        gives = [ord1[0], ord1[2], ord1[4], ord1[7]]
        keeps = [d_mine, x_mine, y_mine, o_mine]
        dd = [rcopy(acc.at[gives[t]], rd.at[t], dd_s.at[t], dd_r.at[t], partner) for t in range(4)]
        x1 = [rcopy(acc.at[d_mine, 0], s1x.at[0], x1_s.at[0], x1_r.at[0], xnb),
              rcopy(acc.at[x_mine, 0], s1x.at[1], x1_s.at[1], x1_r.at[1], xnb)]
        y1 = [rcopy(acc.at[d_mine, 1], s1y.at[0], y1_s.at[0], y1_r.at[0], ynb),
              rcopy(acc.at[y_mine, 1], s1y.at[1], y1_s.at[1], y1_r.at[1], ynb)]
        x2 = rcopy(acc.at[x_mine, 1], s2x, x2_s, x2_r, xnb)
        y2 = rcopy(acc.at[y_mine, 0], s2y, y2_s, y2_r, ynb)

        def far_rows(ci):
            for half in range(2):
                acc[ord1[ci], half] += cols_of(1, res[ord1[ci], half])

        def other_rows(ci):
            chunk = ord1[ci]
            slots = block_wait(ci, ord1, far1)
            for half in range(2):
                val = cols_of(1, stm[slots[half]])
                if ci >= 6:
                    acc[chunk, half] = cols_of(0, res[chunk, half]) + val
                else:
                    acc[chunk, half] += val
            block_next(ci, ord1, ord2, far1)

        def combine(t):
            dd[t].wait_recv()
            acc[keeps[t]] += rd[t]

        with jax.named_scope("p1a"):
            far_rows(0)
            dd[0].start()
            far_rows(1)
            other_rows(2)
            dd[1].start()
        with jax.named_scope("comb0"):
            combine(0)
            x1[0].start()
            y1[0].start()
        with jax.named_scope("p1b"):
            other_rows(3)
            other_rows(4)
            dd[2].start()
        with jax.named_scope("comb1"):
            combine(1)
            x1[1].start()
        with jax.named_scope("p1c"):
            other_rows(5)
        with jax.named_scope("comb2"):
            combine(2)
            y1[1].start()
        with jax.named_scope("p1d"):
            other_rows(6)
            other_rows(7)
            dd[3].start()
        with jax.named_scope("rs2"):
            x1[0].wait_recv()
            acc[y_mine, 0] += s1x[0]
            y2.start()
            y1[0].wait_recv()
            acc[x_mine, 1] += s1y[0]
            x2.start()
        with jax.named_scope("rs3"):
            combine(3)
            x1[1].wait_recv()
            y1[1].wait_recv()
            p0 = acc[o_mine, 0] + s1x[1]
            p1 = acc[o_mine, 1] + s1y[1]
            acc[o_mine, 0] = p0
            acc[o_mine, 1] = p1
        with jax.named_scope("rs4"):
            y2.wait_recv()
            x2.wait_recv()
            p0 = acc[o_mine, 0] + s2y[...]
            p1 = acc[o_mine, 1] + s2x[...]
            auth_out[0] = p0
            auth_out[1] = p1
        with jax.named_scope("ar1"):
            scale = all_sum(square_sums([p0, p1]), sq1, q1_s, q1_r)
        with jax.named_scope("norm1"):
            wide = lane_tile(scale, width)
            for half in range(2):
                val = auth_out[half] * wide
                auth_out[half] = val
                ab[i, half] = val.astype(BF16)
            for c in dd + x1 + y1 + [x2, y2, *h_cps]:
                c.wait_send()

        px, py, pd = ord1[3], ord1[5], ord1[1]
        to_p = rcopy(ab.at[i], ab.at[i], ag_s.at[0], ag_r.at[0], partner)
        to_x = [rcopy(ab.at[i, h], ab.at[i, h], ag_s.at[1 + h], ag_r.at[1 + h], xnb) for h in range(2)]
        to_y = [rcopy(ab.at[i, h], ab.at[i, h], ag_s.at[3 + h], ag_r.at[3 + h], ynb) for h in range(2)]
        rel_y = rcopy(ab.at[px, 0], ab.at[px, 0], ag_s.at[5], ag_r.at[5], ynb)
        rel_x = rcopy(ab.at[py, 1], ab.at[py, 1], ag_s.at[6], ag_r.at[6], xnb)
        fw_x = rcopy(ab.at[px], ab.at[px], ag_s.at[7], ag_r.at[7], partner)
        fw_y = rcopy(ab.at[py], ab.at[py], ag_s.at[8], ag_r.at[8], partner)
        fw_d = rcopy(ab.at[pd], ab.at[pd], ag_s.at[9], ag_r.at[9], partner)
        to_p.start()
        to_x[0].start()
        to_y[1].start()
        to_x[1].start()
        to_y[0].start()

        zero = none_ref[...]

        def rows_of(chunk, half, block):
            return prod_rows(ab[chunk, half], block, zero)

        def resident(chunk):
            return rows_of(chunk, 0, res[chunk, 0]) + rows_of(chunk, 1, res[chunk, 1])

        def add_other(val, first=False):
            for g in range(groups):
                part = val[:, g * span:(g + 1) * span]
                if first:
                    oth_sum[g] = part
                else:
                    oth_sum[g] += part

        def streamed(ci, first=False):
            chunk = ord2[ci]
            slots = block_wait(ci, ord2, far2)
            add_other(rows_of(chunk, 0, stm[slots[0]]) + rows_of(chunk, 1, stm[slots[1]]), first)
            block_next(ci, ord2, ord1, far2)

        with jax.named_scope("p2a"):
            streamed(0, first=True)
        with jax.named_scope("pwait"):
            to_p.wait_recv()
        with jax.named_scope("p2b"):
            streamed(1)
            own_sum[...] = resident(ord2[0]) + resident(ord2[1])
        with jax.named_scope("xwait"):
            to_x[0].wait_recv()
            rel_y.start()
            to_y[1].wait_recv()
            rel_x.start()
        with jax.named_scope("p2c"):
            slots = block_wait(2, ord2, far2) + block_wait(3, ord2, far2)
            add_other(rows_of(ord2[2], 0, stm[slots[0]]) + rows_of(ord2[3], 1, stm[slots[3]]))
            block_next(2, ord2, ord1, far2, 0)
            block_next(3, ord2, ord1, far2, 1)
        with jax.named_scope("xwait2"):
            to_x[1].wait_recv()
            fw_x.start()
            to_y[0].wait_recv()
            fw_y.start()
        with jax.named_scope("p2d"):
            add_other(rows_of(ord2[2], 1, stm[slots[1]]) + rows_of(ord2[3], 0, stm[slots[2]]))
            block_next(2, ord2, ord1, far2, 1)
            block_next(3, ord2, ord1, far2, 0)
        with jax.named_scope("fxwait"):
            fw_x.wait_recv()
        with jax.named_scope("p2e"):
            streamed(4)
        with jax.named_scope("dwait"):
            rel_y.wait_recv()
            rel_x.wait_recv()
            fw_d.start()
            fw_y.wait_recv()
        with jax.named_scope("p2f"):
            streamed(5)
        with jax.named_scope("fdwait"):
            fw_d.wait_recv()
        with jax.named_scope("p2g"):
            z_cps = [rcopy(oth_sum.at[g], zr.at[g], z_s.at[g], z_r.at[g], znb) for g in range(groups)]
            for g in range(groups):
                val = oth_sum[g]
                for q in (6, 7):
                    for half in range(2):
                        val += rows_of(ord2[q], half, res[ord2[q], half, g * span:(g + 1) * span, :])
                oth_sum[g] = val
                z_cps[g].start()

        with jax.named_scope("p2rest"):
            def pair(t, c):
                own_sum[...] += resident(base_x + t) + resident(base_y + t)
                return c
            lax.fori_loop(0, 2, pair, 0)
            slots = block_wait(6, ord2, far2) + block_wait(7, ord2, far2)
            for q in range(4):
                own_sum[...] += rows_of(ord2[6 + q // 2], q % 2, stm[slots[q]])
        with jax.named_scope("zwait"):
            for g in range(groups):
                z_cps[g].wait_recv()
        with jax.named_scope("ar2"):
            val = own_sum[...] + jnp.concatenate([zr[g] for g in range(groups)], axis=1)
            own_sum[...] = val
            scale = all_sum(square_sums([val]), sq2, q2_s, q2_r)
        with jax.named_scope("upd"):
            wt = bt[k]
            hv = lane_tile(1.0 - wt, rows) * (own_sum[...] * lane_tile(scale, rows)) + lane_tile(wt, rows) * vt[...]
            hub_out[...] = hv
            for c in [to_p, *to_x, *to_y, rel_y, rel_x, fw_x, fw_y, fw_d, *z_cps]:
                c.wait_send()

        with jax.named_scope("own"):
            @pl.when(k < sweeps - 1)
            def _():
                send_h(hub_out[...])
                own_far()
                own_near()
        return carry

    lax.fori_loop(0, sweeps, sweep, 0)
    for half in range(2):
        load(ord1[2], half, 4 + half, False).wait()


def solution(mesh):
    def device_fn(adj_tile, pers_piece, restart_wt):
        sweeps, dim = restart_wt.shape
        chunk = pers_piece.shape[0]
        width = chunk // 2
        n_total = float(chunk * mesh.size)
        groups = 6 if chunk % 768 == 0 else 2
        vmem = pl.BlockSpec(memory_space=pltpu.VMEM)
        dma = pltpu.SemaphoreType.DMA
        auth, hub = pl.pallas_call(
            functools.partial(kernel, n_total),
            out_shape=(jax.ShapeDtypeStruct((2, dim, width), F32), jax.ShapeDtypeStruct((dim, chunk), F32)),
            in_specs=[vmem, vmem, pl.BlockSpec(memory_space=pl.ANY)],
            out_specs=(vmem, vmem),
            scratch_shapes=[
                pltpu.VMEM((8, 2, chunk, width), BF16),
                pltpu.VMEM((SLOTS, chunk, width), BF16),
                pltpu.VMEM((dim, chunk), F32),
                pltpu.VMEM((sweeps, dim, 128), F32),
                pltpu.VMEM((2, 2, dim, width), BF16),
                pltpu.VMEM((8, 2, dim, width), BF16),
                pltpu.VMEM((8, 2, dim, width), F32),
                pltpu.VMEM((dim, chunk), F32),
                pltpu.VMEM((groups, dim, chunk // groups), F32),
                pltpu.VMEM((4, 2, dim, width), F32),
                pltpu.VMEM((2, dim, width), F32),
                pltpu.VMEM((2, dim, width), F32),
                pltpu.VMEM((dim, width), F32),
                pltpu.VMEM((dim, width), F32),
                pltpu.VMEM((groups, dim, chunk // groups), F32),
                pltpu.VMEM((16, 128), BF16),
                pltpu.VMEM((8, 128), F32),
                pltpu.VMEM((16, 8, 128), F32),
                pltpu.VMEM((16, 8, 128), F32),
                dma((16,)), dma((SLOTS,)), dma((4,)), dma((4,)), dma((2,)), dma((2,)), dma((2,)), dma((2,)),
                dma, dma, dma, dma, dma((10,)), dma((10,)), dma((groups,)), dma((groups,)), dma((2,)), dma((2,)),
                dma((16,)), dma((16,)), dma((16,)), dma((16,)),
            ],
            compiler_params=pltpu.CompilerParams(vmem_limit_bytes=67043328, has_side_effects=True, collective_id=0),
        )(pers_piece, restart_wt, adj_tile)
        return auth.transpose(0, 2, 1).reshape(chunk, dim), hub.T

    return jax.shard_map(
        device_fn, mesh=mesh,
        in_specs=(P("row", "col"), P(("row", "col"), None), P(None, None)),
        out_specs=(P(("col", "row"), None), P(("row", "col"), None)), check_vma=False)
```
